128 devices in a mesh: turn: 8 (over z, core), group: 4 (over x), head: 4 (over y).
Axes of the slice: x: 4, y: 4, z: 4, core: 2. Of those that a mesh axis runs over, the one named last changes fastest.
Arguments:
- hidden: bfloat16 [32, 4, 16, 16, 3584], P('turn', 'group', None, None, 'head'), may hold values from -6 to 6
- dense_weight: bfloat16 [3584, 3584], P('head'), may hold values from -0.09375 to 0.09375
- dense_bias: float32 [3584], replicated, may hold values from -3 to 3
- score_weight: float32 [3584], replicated, may hold values from -0.09375 to 0.09375
- valid_turns: int32 [4, 16], P('group'), may hold values from 8 to 32
- terminal_turn: int32 [4, 16], P('group'), may hold values from 0 to 31, as said below
- terminal_value: int32 [4, 16], P('group'), may hold values from -3 to 3
- gamma_den: int32 [4, 16], P('group'), may hold values from 112 to 128
- gamma_drop: int32 [4, 16], P('group'), may hold values from 1 to 4
Outputs:
- returns: float32 [32, 4, 16], P(('turn', 'head'), 'group')
- advantages: float32 [32, 4, 16], P(('turn', 'head'), 'group')
The draws below stay inside these ranges and needn't reach their ends.
Inputs may be any that keep to these rules, and one draw needn't show every extreme that they name: terminal_turn is below valid_turns of the same rollout.
All inputs are finite; a program needn't handle non-finite values.
Results may differ from the reference program's by a relative error of at most 0.0003.
Values may be sent and summed in bfloat16 or wider, within the bound.
No kernel may reach another device: no remote copies, remote signals or barrier semaphores. Data moves between devices by JAX's collectives and lax.ppermute only.
A program may use at most 128 MiB of HBM per device.

```python
import jax
import jax.numpy as jnp
from jax import lax

D = 3584
TOK_TURN = 16
ROLL = 16
TURNS = 32
PROMPTS = 4


def turn_pair(key):
    counts = jax.random.randint(jax.random.fold_in(key, 11), (PROMPTS, ROLL), TURNS // 4, TURNS + 1)
    spread = jax.random.randint(jax.random.fold_in(key, 12), (PROMPTS, ROLL), 0, 1048576)
    return (counts.astype(jnp.int32), (spread % counts).astype(jnp.int32))


def draw_valid_turns(key, part):
    return turn_pair(key)[0]


def draw_terminal_turn(key, part):
    return turn_pair(key)[1]


def set_ends(array, key, least, high):
    index_at = [jax.random.randint(jax.random.fold_in(key, axis), (), 0, length) for axis, length in enumerate(array.shape)]
    longest = array.shape.index(max(array.shape))
    neighbour = index_at[:longest] + [(index_at[longest] + 1) % array.shape[longest]] + index_at[longest + 1:]
    return array.at[tuple(index_at)].set(least).at[tuple(neighbour)].set(high)


def levels(rng, extent, shards, low, top_value):
    def one(position, parts):
        draws = jax.random.uniform(jax.random.fold_in(jax.random.fold_in(rng, 6), position), (parts,), jnp.float32, low / len(shards), top_value / len(shards))
        return jnp.repeat(jnp.exp(draws), extent[position] // parts).reshape((-1,) + (1,) * (len(extent) - position - 1))

    level = one(*shards[0])
    for cut in shards[1:]:
        level = level * one(*cut)
    return level


def bell_draw(key, dims, scale, limit, cuts=(), held_as=jnp.bfloat16):
    array = jax.random.normal(key, dims, jnp.float32) * scale
    if len(cuts) > 0:
        array = levels(key, dims, cuts, -0.22, 0.18) * array
    return jnp.clip(array, min=-limit, max=limit).astype(held_as)


def setup_inputs(seed: int = 0) -> dict:
    arg_keys = jax.random.split(jax.random.key(seed), 10)
    hidden = bell_draw(arg_keys[0], (TURNS, PROMPTS, ROLL, TOK_TURN, D), 1.0, 6.0, ((0, 8), (1, 4), (4, 4)))
    dense_weight = bell_draw(arg_keys[1], (D, D), D ** -0.5, 0.09375, ((0, 4),))
    dense_bias = bell_draw(arg_keys[2], (D,), 0.5, 3.0, (), jnp.float32)
    score_weight = bell_draw(arg_keys[3], (D,), D ** -0.5, 0.09375, (), jnp.float32)
    valid_turns = draw_valid_turns(jax.random.fold_in(arg_keys[9], 71), 0)
    terminal_turn = draw_terminal_turn(jax.random.fold_in(arg_keys[9], 71), 0)
    terminal_value = set_ends(jax.random.randint(arg_keys[6], (PROMPTS, ROLL), -3, 4), jax.random.fold_in(arg_keys[6], 1), -3, 3).astype(jnp.int32)
    gamma_den = set_ends(jax.random.randint(arg_keys[7], (PROMPTS, ROLL), 112, 129), jax.random.fold_in(arg_keys[7], 1), 112, 128).astype(jnp.int32)
    gamma_drop = set_ends(jax.random.randint(arg_keys[8], (PROMPTS, ROLL), 1, 5), jax.random.fold_in(arg_keys[8], 1), 1, 4).astype(jnp.int32)
    return dict(hidden=hidden, dense_weight=dense_weight, dense_bias=dense_bias, score_weight=score_weight, valid_turns=valid_turns, terminal_turn=terminal_turn, terminal_value=terminal_value, gamma_den=gamma_den, gamma_drop=gamma_drop)


def reference(hidden, dense_weight, dense_bias, score_weight, valid_turns, terminal_turn, terminal_value, gamma_den, gamma_drop):

    def turn_score(states):
        rows = states.reshape(-1, D)
        pre = jnp.dot(rows, dense_weight, preferred_element_type=jnp.float32)
        active = jnp.tanh(pre + dense_bias)
        score = jnp.dot(active, score_weight, precision=lax.Precision.HIGHEST)
        return score.reshape(PROMPTS, ROLL, TOK_TURN).mean(axis=-1)
    dense = lax.map(turn_score, hidden)
    positions = jnp.arange(TURNS, dtype=jnp.int32)[:, None, None]
    valid = positions < valid_turns[None]
    hits = (positions == terminal_turn[None]).astype(jnp.float32)
    reward = jnp.where(valid, dense + 0.25 * terminal_value[None].astype(jnp.float32) * hits, 0.0)
    gamma = (gamma_den - gamma_drop).astype(jnp.float32) / gamma_den.astype(jnp.float32)

    def backward(carry, current):
        value = current + gamma * carry
        return (value, value)
    _, returns = lax.scan(backward, jnp.zeros((PROMPTS, ROLL), jnp.float32), reward, reverse=True)
    weights = valid.astype(jnp.float32)
    count = lax.optimization_barrier(jnp.sum(valid_turns, axis=1)).astype(jnp.float32)
    mean = lax.optimization_barrier(jnp.sum(weights * returns, axis=(0, 2))) / count
    centered = returns - mean[None, :, None]
    var = lax.optimization_barrier(jnp.sum(weights * centered * centered, axis=(0, 2))) / count
    advantages = weights * centered / jnp.sqrt(var[None, :, None] + 1e-06)
    return (returns, advantages)
```

```python
import jax
import jax.numpy as jnp
from jax import lax
from jax.sharding import Mesh, PartitionSpec as P


def shift(axis, by):
    n = lax.axis_size(axis)
    return [(i, (i + by) % n) for i in range(n)]


def block(array, index, size, axis):
    return lax.dynamic_slice_in_dim(array, index * size, size, axis)


def spread(value, axis):
    n = lax.axis_size(axis)
    copies = jnp.broadcast_to(value, (n, *value.shape))
    return lax.all_to_all(copies, axis, split_axis=0, concat_axis=0, tiled=True)


def local(
    hidden,
    dense_weight,
    dense_bias,
    score_weight,
    valid_turns,
    terminal_turn,
    terminal_value,
    gamma_den,
    gamma_drop,
):
    turn_dev, p_dev, roll, tok, depth = hidden.shape
    width = dense_weight.shape[1]
    half, quarter = width // 2, width // 4
    rows = roll * tok
    heads = lax.axis_size("head")
    y = lax.axis_index("head")
    x = lax.axis_index("group")
    z = lax.axis_index("z")
    core = lax.axis_index("core")
    side = lax.rem(y, 2)

    nx, nz = lax.axis_size("group"), lax.axis_size("z")
    chips = nx * nz
    unit_a = (depth // chips) * 4 // 7
    unit_b = depth // chips - unit_a
    top = unit_a * chips

    def piece(which):
        col = (which * 2 + core) * quarter
        a = lax.dynamic_slice(dense_weight, ((z * nx + x) * unit_a, col), (unit_a, quarter))
        b = lax.dynamic_slice(dense_weight, (top + (x * nz + z) * unit_b, col), (unit_b, quarter))
        return jnp.concatenate([a, b])

    near, far = piece(1 - side), piece(side)
    w_in = jnp.stack(
        [
            lax.ppermute(near, "head", shift("head", 1)),
            lax.ppermute(near, "head", shift("head", heads - 1)),
            lax.ppermute(far, "head", shift("head", 2)),
        ]
    )

    states = hidden.reshape(turn_dev, rows, depth)

    def turn(offset):
        return lax.dynamic_slice_in_dim(states, lax.rem(y + offset, heads), 1, 0)

    t0, t1, t2, t3 = (turn(k) for k in range(4))
    below = lax.ppermute(jnp.concatenate([t1, t2]), "head", shift("head", 1))
    above = lax.ppermute(jnp.concatenate([t3, t0]), "head", shift("head", heads - 1))
    own = jnp.concatenate([t0, t1])

    pa, pb = w_in[:, :unit_a], w_in[:, unit_a:]
    pa = spread(pa, "group")
    pb = spread(pb, "z")
    pa = spread(pa, "z")
    pb = spread(pb, "group")

    far0 = lax.ppermute(below[1], "head", shift("head", 1))
    far1 = lax.ppermute(above[0], "head", shift("head", heads - 1))
    beyond = jnp.stack([far0, far1])

    qa = lax.ppermute(pa, "core", [(0, 1), (1, 0)])
    qb = lax.ppermute(pb, "core", [(0, 1), (1, 0)])

    def dot(a, b):
        return jnp.dot(a, b, preferred_element_type=jnp.float32)

    others = [v.reshape(2 * rows, depth) for v in (below, above, beyond)]

    def score(a, b, which):
        col = (side * 2 + which) * quarter
        pre = dot(own.reshape(2 * rows, depth), lax.dynamic_slice(dense_weight, (0, col), (depth, quarter)))
        for k in range(3):
            w = jnp.concatenate([a[:, :, k].reshape(top, quarter), b[:, :, k].reshape(depth - top, quarter)])
            pre = pre + dot(others[k], w)
        bias = lax.dynamic_slice_in_dim(dense_bias, col, quarter)
        weight = lax.dynamic_slice_in_dim(score_weight, col, quarter)
        return jnp.sum(jnp.tanh(pre + bias) * weight, axis=-1)

    partial = score(pa, pb, core) + score(qa, qb, 1 - core)
    part = partial.reshape(2, roll, tok).sum(axis=-1) / tok

    every = spread(part.reshape(1, -1), ("z", "core", "head"))
    every = every.reshape(-1, heads, 2, roll)
    dense = every[:, :, 0] + jnp.roll(every[:, :, 1], 1, axis=1)
    dense = dense.reshape(-1, p_dev, roll)
    turns = dense.shape[0]

    positions = jnp.arange(turns, dtype=jnp.int32)[:, None, None]
    valid = positions < valid_turns[None]
    hits = (positions == terminal_turn[None]).astype(jnp.float32)
    reward = jnp.where(valid, dense + 0.25 * terminal_value[None].astype(jnp.float32) * hits, 0.0)
    gamma = (gamma_den - gamma_drop).astype(jnp.float32) / gamma_den.astype(jnp.float32)
    returns, factor, step = reward, gamma[None], 1
    while step < turns:
        later = jnp.concatenate([returns[step:], jnp.zeros_like(returns[:step])])
        returns = returns + factor * later
        factor, step = factor * factor, step * 2
    weights = valid.astype(jnp.float32)
    count = jnp.sum(valid_turns, axis=1).astype(jnp.float32)
    mean = jnp.sum(weights * returns, axis=(0, 2)) / count
    centered = returns - mean[None, :, None]
    var = jnp.sum(weights * centered * centered, axis=(0, 2)) / count
    advantages = weights * centered / jnp.sqrt(var[None, :, None] + 1e-06)
    here = lax.axis_index(("z", "core", "head"))
    return tuple(lax.dynamic_slice_in_dim(v, here, 1, 0) for v in (returns, advantages))


def solution(mesh):
    sizes = mesh.devices.shape
    split = Mesh(
        mesh.devices.reshape(sizes[0] // 2, 2, *sizes[1:]), ("z", "core", *mesh.axis_names[1:])
    )
    turn = ("z", "core")
    small = P("group", None)
    in_specs = (P(turn, "group", None, None, "head"), P("head", None), P(), P(), *(small,) * 5)
    out = P((*turn, "head"), "group", None)
    return jax.shard_map(local, mesh=split, in_specs=in_specs, out_specs=(out, out), check_vma=False)
```
